32 devices in a mesh: left: 8 (over y, x, core), right: 4 (over z).
Axes of the slice: x: 2, y: 2, z: 4, core: 2. Of those that a mesh axis runs over, the one named last changes fastest.
Arguments:
- signal: float32 [256, 256, 1024], P(None, 'left', 'right'), may hold values from -6 to 6
- symbol_x: float32 [256], replicated, may hold values from 0.3 to 3
- symbol_y: float32 [256], replicated, may hold values from 0.3 to 3
- symbol_z: float32 [1024], replicated, may hold values from 0.3 to 3
Outputs:
- spectrum: float32 [128, 128, 512], P('left', 'right')
The draws below stay inside these ranges and needn't reach their ends.
All inputs are finite; a program needn't handle non-finite values.
Results may differ from the reference program's by a relative error of at most 0.000096.
Values sent between devices are 32-bit elements; how exact they have to be, the bound alone decides.
A program may use at most 128 MiB of HBM per device.

```python
import jax
import jax.numpy as jnp
from jax import lax

GRID_X = 256
GRID_Y = 256
GRID_Z = 1024


def steps_of(stream_key, extent, shards, smallest, largest):
    gain = 1.0
    for position, blocks in shards:
        steps = jax.random.uniform(jax.random.fold_in(jax.random.fold_in(stream_key, 6), position), (blocks,), jnp.float32, smallest / len(shards), largest / len(shards))
        gain = gain * jnp.repeat(jnp.exp(steps), extent[position] // blocks).reshape((-1,) + (1,) * (len(extent) - 1 - position))
    return gain


def normal_values(stream_key, extent, spread, most, split=(), dtype=jnp.bfloat16):
    level = steps_of(stream_key, extent, split, -0.22, 0.18) if split else 1.0
    result = jax.random.normal(stream_key, extent, jnp.float32) * spread * level
    return jnp.minimum(jnp.maximum(result, -most), most).astype(dtype)


def setup_inputs(seed: int = 0) -> dict:
    splits = jax.random.split(jax.random.key(seed), 5)
    return {
        "signal": normal_values(splits[0], (GRID_X, GRID_Y, GRID_Z), 1.0, 6.0, ((1, 8), (2, 4)), jnp.float32),
        "symbol_x": jnp.clip(jax.random.uniform(splits[1], (GRID_X,), jnp.float32, 0.3, 3.0), 0.3, 3.0),
        "symbol_y": jnp.clip(jax.random.uniform(splits[2], (GRID_Y,), jnp.float32, 0.3, 3.0), 0.3, 3.0),
        "symbol_z": jnp.clip(jax.random.uniform(splits[3], (GRID_Z,), jnp.float32, 0.3, 3.0), 0.3, 3.0),
    }


def transform_table(count):
    rank = jnp.arange(count)
    angle = (jnp.pi / (4 * count)) * (((2 * rank[:, None] + 1) * (2 * rank[None, :] + 1)) % (8 * count)).astype(jnp.float32)
    return jnp.cos(angle) * (2.0 / count) ** 0.5


def transform_dim(values, dim):
    moved = jnp.tensordot(values, transform_table(values.shape[dim]), axes=([dim], [0]), precision=lax.Precision.HIGHEST)
    return jnp.moveaxis(moved, -1, dim)


def reference(signal, symbol_x, symbol_y, symbol_z):
    spectrum = signal
    spectrum = transform_dim(spectrum, 0)
    spectrum = lax.slice_in_dim(spectrum, 0, GRID_X // 2, axis=0)
    spectrum = transform_dim(spectrum, 1)
    spectrum = lax.slice_in_dim(spectrum, 0, GRID_Y // 2, axis=1)
    spectrum = transform_dim(spectrum, 2)
    spectrum = lax.slice_in_dim(spectrum, 0, GRID_Z // 2, axis=2)
    symbol = symbol_x[:GRID_X // 2][:, None, None] + symbol_y[:GRID_Y // 2][None, :, None] + symbol_z[:GRID_Z // 2][None, None, :]
    spectrum = spectrum * ((1.0 - 0.2 * symbol) / (1.0 + 0.2 * symbol))
    return spectrum
```

```python
import functools

import jax
import jax.numpy as jnp
import numpy as np
from jax import lax
from jax.experimental import pallas as pl
from jax.experimental.pallas import tpu as pltpu
from jax.sharding import PartitionSpec as P

MESH = pl.DeviceIdType.MESH
LANES = 128
ROWS = 8
AHEAD = 2
REST = 32


def kept_table(count):
    rank = np.arange(count)
    odd = 2 * rank + 1
    angle = np.pi / (4 * count) * ((odd[:, None] * odd[None, : count // 2]) % (8 * count))
    return np.cos(angle) * (2.0 / count) ** 0.5


def half_band_basis(count, keep):
    at = np.arange(1, count)
    off = at * (count - at) / 2.0
    columns = np.linalg.eigh(np.diag(off, 1) + np.diag(off, -1))[1][:, ::-1][:, :keep]
    peak = columns[np.abs(columns).argmax(axis=0), np.arange(keep)]
    return columns * np.where(peak < 0, -1.0, 1.0)


def two_halves(table):
    high = table.astype(np.float32).astype(jnp.bfloat16)
    rest = table - high.astype(np.float64)
    return np.stack([high, rest.astype(np.float32).astype(jnp.bfloat16)])


def split(values):
    high = values.astype(jnp.bfloat16)
    return high, (values - high.astype(jnp.float32)).astype(jnp.bfloat16)


def product(first, second):
    dot = functools.partial(jnp.dot, preferred_element_type=jnp.float32)
    return dot(first[0], second[0]) + (dot(first[0], second[1]) + dot(first[1], second[0]))


def kernel(
    lefts, rights, group, cuts,
    signal, table_x, table_y, table_v, table_w, symbol_x, symbol_y, symbol_z, out,
    held, tx, ty, tv, tw, spread, first, lines, second, pencils, done,
    held_sem, table_sem, send0, recv0, send1, recv1, send2, recv2, out_sem,
):
    left, right = lax.axis_index("left"), lax.axis_index("right")
    tiles, blocks, size_x = held.shape[0], held.shape[1], held.shape[2]
    modes_x = size_x // 2
    slots = lines.shape[2]
    share_x = done.shape[0]
    size_y = lefts * tiles * ROWS
    modes_y = size_y // 2
    share_y = modes_y // rights
    groups = share_x // group
    unit = group + 1
    rest = LANES // group
    begins = [sum(cuts[:k]) for k in range(len(cuts))]
    lane_group = lax.broadcasted_iota(jnp.int32, (ROWS, LANES), 1) // rest

    def tile_copy(t, b):
        return pltpu.make_async_copy(
            signal.at[:, pl.ds(t * ROWS, ROWS), pl.ds(b * LANES, LANES)],
            held.at[t, b], held_sem.at[t, b])

    copy_x = pltpu.make_async_copy(table_x, tx, table_sem.at[0])
    copy_v = pltpu.make_async_copy(table_v, tv, table_sem.at[1])
    copy_y = pltpu.make_async_copy(table_y, ty, table_sem.at[2])
    copy_w = pltpu.make_async_copy(table_w, tw, table_sem.at[3])
    copy_x.start()
    for t in range(min(AHEAD, tiles)):
        for b in range(blocks):
            tile_copy(t, b).start()
    copy_v.start()

    barrier = pltpu.get_barrier_semaphore()
    for o in range(1, lefts):
        pl.semaphore_signal(barrier, 1, device_id=(lax.bitwise_xor(left, o), right), device_id_type=MESH)
    for o in range(1, rights):
        pl.semaphore_signal(barrier, 1, device_id=(left, lax.bitwise_xor(right, o)), device_id_type=MESH)

    copy_x.wait()
    copy_v.wait()

    def send_tile(t, o):
        to = lax.bitwise_xor(left, o)
        return pltpu.make_async_remote_copy(
            src_ref=first.at[t, pl.ds(to * slots, cuts[0])],
            dst_ref=lines.at[left, t, pl.ds(0, cuts[0])],
            send_sem=send0.at[o, t], recv_sem=recv0.at[o, t],
            device_id=(to, right), device_id_type=MESH)

    def send_left(g, k, o):
        to = lax.bitwise_xor(left, o)
        at = g * unit + begins[k]
        return pltpu.make_async_remote_copy(
            src_ref=first.at[:, pl.ds(to * slots + at, cuts[k])],
            dst_ref=lines.at[left, :, pl.ds(at, cuts[k])],
            send_sem=send1.at[o, g, k], recv_sem=recv1.at[o, g, k],
            device_id=(to, right), device_id_type=MESH)

    def send_right(g, k, o):
        to = lax.bitwise_xor(right, o)
        at = g * unit + begins[k]
        return pltpu.make_async_remote_copy(
            src_ref=second.at[pl.ds(at, cuts[k]), pl.ds(pl.multiple_of(to * share_y, share_y), share_y), :],
            dst_ref=pencils.at[right, pl.ds(at, cuts[k])],
            send_sem=send2.at[o, g, k], recv_sem=recv2.at[o, g, k],
            device_id=(left, to), device_id_type=MESH)

    def result_copy(g):
        return pltpu.make_async_copy(
            done.at[pl.ds(g * group, group)], out.at[pl.ds(g * group, group)], out_sem.at[g])

    def stage1(t, carry):
        for b in range(blocks):
            tile_copy(t, b).wait()

        @pl.when(t + AHEAD < tiles)
        def _():
            for b in range(blocks):
                tile_copy(t + AHEAD, b).start()

        parts = []
        for y in range(ROWS):
            values = jnp.concatenate(
                [held.at[t, b].reshape(size_x * ROWS, LANES)[pl.ds(y, size_x, stride=ROWS), :] for b in range(blocks)],
                axis=1)
            parts.append(product((tx[0], tx[1]), split(values)))
        result = product(split(jnp.concatenate(parts, axis=0)), (tv[0], tv[1]))
        for y in range(ROWS):
            for b in range(2):
                spread.at[b].reshape(modes_x * ROWS, LANES)[pl.ds(y, modes_x, stride=ROWS), :] = (
                    result[y * modes_x : (y + 1) * modes_x, b * LANES : (b + 1) * LANES])

        def place(n, carry):
            packed = spread[1, n * group]
            for j in range(1, group):
                packed = jnp.where(lane_group == j, spread[1, n * group + j], packed)
            first[t, n * unit] = packed
            for j in range(group):
                first[t, n * unit + 1 + j] = spread[0, n * group + j]
            return carry

        lax.fori_loop(0, modes_x // group, place, 0, unroll=4)

        @pl.when(t == 0)
        def _():
            pl.semaphore_wait(barrier, lefts + rights - 2)

        for o in range(lefts - 1, 0, -1):
            send_tile(t, o).start()
        return carry

    lax.fori_loop(0, tiles, stage1, 0)

    def start1(g, carry):
        for k in range(len(cuts)):
            def start():
                for o in range(lefts - 1, 0, -1):
                    send_left(g, k, o).start()

            if k == 0:
                pl.when(g > 0)(start)
            else:
                start()
        return carry

    lax.fori_loop(0, groups, start1, 0)
    copy_y.start()
    copy_w.start()

    def own1(s, carry):
        for t in range(tiles):
            lines[left, t, s] = first[t, left * slots + s]
        return carry

    lax.fori_loop(0, slots, own1, 0)
    copy_y.wait()
    copy_w.wait()

    pick = lax.broadcasted_iota(jnp.int32, (share_y, symbol_y.shape[1]), 1) == (
        right * share_y + lax.broadcasted_iota(jnp.int32, (share_y, symbol_y.shape[1]), 0))
    part_y = jnp.sum(jnp.where(pick, symbol_y[...], 0.0), axis=1, keepdims=True)
    modes_z = done.shape[2]
    wide_group = lax.broadcasted_iota(jnp.int32, (share_y, LANES), 1) // rest

    def stage23(g, carry):
        @pl.when(g < groups)
        def _():
            for k in range(len(cuts)):
                def wait_left():
                    for o in range(lefts - 1, 0, -1):
                        send_left(g, k, o).wait_recv()

                if k == 0:
                    pl.when(g > 0)(wait_left)

                    @pl.when(g == 0)
                    def _():
                        for t in range(tiles):
                            for o in range(1, lefts):
                                send_tile(t, o).wait_recv()
                else:
                    wait_left()

                at = g * unit + begins[k]
                values = jnp.concatenate(
                    [lines[:, :, at + s].reshape(size_y, LANES) for s in range(cuts[k])], axis=1)
                result = product((ty[0], ty[1]), split(values))
                for s in range(cuts[k]):
                    second[at + s] = result[:, s * LANES : (s + 1) * LANES]
                for o in range(rights - 1, 0, -1):
                    send_right(g, k, o).start()
                for s in range(cuts[k]):
                    pencils[right, at + s] = second[at + s, pl.ds(pl.multiple_of(right * share_y, share_y), share_y), :]

        @pl.when(g >= 1)
        def _():
            d = g - 1
            for k in range(len(cuts)):
                for o in range(1, rights):
                    send_right(d, k, o).wait_recv()
            columns = []
            for p in range(rights):
                columns.append(pencils[p, pl.ds(d * unit + 1, group)].reshape(group * share_y, LANES))
                packed = pencils[p, d * unit]
                columns.append(jnp.concatenate([jnp.where(wide_group == j, packed, 0.0) for j in range(group)], axis=0))
            result = product(split(jnp.concatenate(columns, axis=1)), (tw[0], tw[1]))
            for s in range(group):
                x = d * group + s
                symbol = (symbol_x[left * share_x + x] + part_y) + symbol_z[:, :modes_z]
                done[x] = result[s * share_y : (s + 1) * share_y] * ((1.0 - 0.2 * symbol) / (1.0 + 0.2 * symbol))
            result_copy(d).start()
        return carry

    lax.fori_loop(0, groups + 1, stage23, 0)

    for t in range(tiles):
        for o in range(1, lefts):
            send_tile(t, o).wait_send()

    def finish(g, carry):
        for k in range(len(cuts)):
            def wait_left():
                for o in range(1, lefts):
                    send_left(g, k, o).wait_send()

            if k == 0:
                pl.when(g > 0)(wait_left)
            else:
                wait_left()
            for o in range(1, rights):
                send_right(g, k, o).wait_send()
        result_copy(g).wait()
        return carry

    lax.fori_loop(0, groups, finish, 0)


def body(lefts, rights, signal, symbol_x, symbol_y, symbol_z):
    size_x, own_y, own_z = signal.shape
    size_y, size_z = own_y * lefts, own_z * rights
    modes_x, modes_y, modes_z = size_x // 2, size_y // 2, size_z // 2
    share_x, share_y = modes_x // lefts, modes_y // rights
    blocks, tiles = own_z // LANES, own_y // ROWS
    group = LANES // REST
    groups = share_x // group
    slots = share_x + groups
    cuts = (2, group - 1)
    basis = half_band_basis(own_z, LANES + REST)
    table_x = two_halves(kept_table(size_x).T)
    table_y = two_halves(kept_table(size_y).T)
    table_v = two_halves(np.concatenate([basis[:, :LANES]] + [basis[:, LANES:]] * group, axis=1))
    rows = np.einsum("ic,pik->pck", basis, kept_table(size_z).reshape(rights, own_z, modes_z))
    table_w = two_halves(
        np.concatenate([rows[:, :LANES]] + [rows[:, LANES:]] * group, axis=1).reshape(rights * 2 * LANES, modes_z))
    vmem = pl.BlockSpec(memory_space=pltpu.VMEM)
    any_ = pl.BlockSpec(memory_space=pl.ANY)
    smem = pl.BlockSpec(memory_space=pltpu.SMEM)
    dma = pltpu.SemaphoreType.DMA
    return pl.pallas_call(
        functools.partial(kernel, lefts, rights, group, cuts),
        out_shape=jax.ShapeDtypeStruct((share_x, share_y, modes_z), jnp.float32),
        in_specs=[any_] * 5 + [smem, vmem, vmem],
        out_specs=any_,
        scratch_shapes=[
            pltpu.VMEM((tiles, blocks, size_x, ROWS, LANES), jnp.float32),
            pltpu.VMEM(table_x.shape, jnp.bfloat16),
            pltpu.VMEM(table_y.shape, jnp.bfloat16),
            pltpu.VMEM(table_v.shape, jnp.bfloat16),
            pltpu.VMEM(table_w.shape, jnp.bfloat16),
            pltpu.VMEM((2, modes_x, ROWS, LANES), jnp.float32),
            pltpu.VMEM((tiles, lefts * slots, ROWS, LANES), jnp.float32),
            pltpu.VMEM((lefts, tiles, slots, ROWS, LANES), jnp.float32),
            pltpu.VMEM((slots, modes_y, LANES), jnp.float32),
            pltpu.VMEM((rights, slots, share_y, LANES), jnp.float32),
            pltpu.VMEM((share_x, share_y, modes_z), jnp.float32),
            dma((tiles, blocks)),
            dma((4,)),
            dma((lefts, tiles)),
            dma((lefts, tiles)),
            dma((lefts, groups, len(cuts))),
            dma((lefts, groups, len(cuts))),
            dma((rights, groups, len(cuts))),
            dma((rights, groups, len(cuts))),
            dma((groups,)),
        ],
        compiler_params=pltpu.CompilerParams(
            collective_id=0, has_side_effects=True, vmem_limit_bytes=62 * 2**20),
    )(signal, table_x, table_y, table_v, table_w, symbol_x, symbol_y[None, :], symbol_z[None, :])


def solution(mesh):
    lefts, rights = mesh.shape["left"], mesh.shape["right"]
    in_specs = (P(None, "left", "right"), P(), P(), P())
    out_specs = P("left", "right", None)
    return jax.shard_map(
        functools.partial(body, lefts, rights), mesh=mesh, in_specs=in_specs, out_specs=out_specs, check_vma=False)
```

```python
import functools

import jax
import jax.numpy as jnp
import numpy as np
from jax import lax
from jax.experimental import pallas as pl
from jax.experimental.pallas import tpu as pltpu
from jax.sharding import PartitionSpec as P

MESH = pl.DeviceIdType.MESH
LANES = 128
ROWS = 8
AHEAD = 2
EARLY = 2
REST = 32


def kept_table(count):
    rank = np.arange(count)
    odd = 2 * rank + 1
    angle = np.pi / (4 * count) * ((odd[:, None] * odd[None, : count // 2]) % (8 * count))
    return np.cos(angle) * (2.0 / count) ** 0.5


def half_band_basis(count, keep):
    at = np.arange(1, count)
    off = at * (count - at) / 2.0
    columns = np.linalg.eigh(np.diag(off, 1) + np.diag(off, -1))[1][:, ::-1][:, :keep]
    peak = columns[np.abs(columns).argmax(axis=0), np.arange(keep)]
    return columns * np.where(peak < 0, -1.0, 1.0)


def two_halves(table):
    high = table.astype(np.float32).astype(jnp.bfloat16)
    rest = table - high.astype(np.float64)
    return np.stack([high, rest.astype(np.float32).astype(jnp.bfloat16)])


def split(values):
    high = values.astype(jnp.bfloat16)
    return high, (values - high.astype(jnp.float32)).astype(jnp.bfloat16)


def product(first, second):
    dot = functools.partial(jnp.dot, preferred_element_type=jnp.float32)
    rows = first.shape[0] // 2
    both = dot(first, second[0])
    return both[:rows] + (dot(first[:rows], second[1]) + both[rows:])


def stacked(values):
    return jnp.concatenate(split(values), axis=0)


def kernel(
    lefts, rights, group, cuts,
    signal, table_x, table_y, table_v, table_w, symbol_x, symbol_y, symbol_z, out,
    held, halves, tx, ty, tv, tw, first, lines, second, pencils, done,
    held_sem, table_sem, sent_left, sent_right, came_left, came_right, out_sem,
):
    left, right = lax.axis_index("left"), lax.axis_index("right")
    tiles, blocks, size_x = held.shape[0], held.shape[1], held.shape[2]
    groups, unit = first.shape[1], first.shape[2]
    share_x = done.shape[0]
    size_y = lefts * tiles * ROWS
    modes_y = size_y // 2
    share_y = modes_y // rights
    rest = LANES // group
    rows_g = group * lefts
    early = min(EARLY, groups)
    begins = [sum(cuts[:k]) for k in range(len(cuts))]
    pieces = range(len(cuts))
    lane_group = lax.broadcasted_iota(jnp.int32, (lefts, LANES), 1) // rest

    def tile_copy(t, b):
        return pltpu.make_async_copy(
            signal.at[:, pl.ds(t * ROWS, ROWS), pl.ds(b * LANES, LANES)],
            held.at[t, b], held_sem.at[t, b])

    copy_x = pltpu.make_async_copy(table_x, tx, table_sem.at[0])
    copy_v = pltpu.make_async_copy(table_v, tv, table_sem.at[1])
    copy_y = pltpu.make_async_copy(table_y, ty, table_sem.at[2])
    copy_w = pltpu.make_async_copy(table_w, tw, table_sem.at[3])
    copy_x.start()
    for t in range(min(AHEAD, tiles)):
        for b in range(blocks):
            tile_copy(t, b).start()
    copy_v.start()

    barrier = pltpu.get_barrier_semaphore()
    for o in range(1, lefts):
        pl.semaphore_signal(barrier, 1, device_id=(lax.bitwise_xor(left, o), right), device_id_type=MESH)
    for o in range(1, rights):
        pl.semaphore_signal(barrier, 1, device_id=(left, lax.bitwise_xor(right, o)), device_id_type=MESH)

    copy_x.wait()
    copy_v.wait()

    def send_tile(t, g, k, o):
        to = lax.bitwise_xor(left, o)
        return pltpu.make_async_remote_copy(
            src_ref=first.at[t, g, pl.ds(begins[k], cuts[k]), to],
            dst_ref=lines.at[left, t, pl.ds(g * unit + begins[k], cuts[k])],
            send_sem=sent_left.at[0], recv_sem=came_left.at[g, k],
            device_id=(to, right), device_id_type=MESH)

    def send_left(g, k, o):
        to = lax.bitwise_xor(left, o)
        return pltpu.make_async_remote_copy(
            src_ref=first.at[:, g, pl.ds(begins[k], cuts[k]), to],
            dst_ref=lines.at[left, :, pl.ds(g * unit + begins[k], cuts[k])],
            send_sem=sent_left.at[0], recv_sem=came_left.at[g, k],
            device_id=(to, right), device_id_type=MESH)

    def send_right(g, k, o):
        to = lax.bitwise_xor(right, o)
        at = g * unit + begins[k]
        return pltpu.make_async_remote_copy(
            src_ref=second.at[pl.ds(at, cuts[k]), pl.ds(pl.multiple_of(to * share_y, share_y), share_y), :],
            dst_ref=pencils.at[right, pl.ds(at, cuts[k])],
            send_sem=sent_right.at[0], recv_sem=came_right.at[o, g],
            device_id=(left, to), device_id_type=MESH)

    def all_left(k_at, k_count, recv):
        part = lines.at[pl.ds(0, lefts - 1), :, pl.ds(k_at, k_count)]
        return pltpu.make_async_remote_copy(
            src_ref=part, dst_ref=part, send_sem=sent_left.at[0], recv_sem=recv,
            device_id=(lax.bitwise_xor(left, 1), right), device_id_type=MESH)

    def wait_left(g, k):
        all_left(g * unit + begins[k], cuts[k], came_left.at[g, k]).wait_recv()

    def wait_right(g, o):
        part = pencils.at[0, pl.ds(g * unit, unit)]
        pltpu.make_async_remote_copy(
            src_ref=part, dst_ref=part, send_sem=sent_right.at[0], recv_sem=came_right.at[o, g],
            device_id=(left, lax.bitwise_xor(right, o)), device_id_type=MESH).wait_recv()

    def result_copy(g):
        return pltpu.make_async_copy(
            done.at[pl.ds(g * group, group)], out.at[pl.ds(g * group, group)], out_sem.at[g])

    def transform(t, low, high, piece):
        parts = []
        for y in range(ROWS):
            parts.append(product(tx[pl.ds(2 * low * rows_g, 2 * (high - low) * rows_g), :], piece(y)))
        result = product(stacked(jnp.concatenate(parts, axis=0)), (tv[0], tv[1]))
        for y in range(ROWS):
            for g in range(low, high):
                view = first.at[t, g].reshape(unit * lefts * ROWS, LANES)
                packed = None
                for j in range(group):
                    at = ((y * (high - low) + g - low) * group + j) * lefts
                    rows = result[at : at + lefts]
                    view[pl.ds((1 + j) * lefts * ROWS + y, lefts, stride=ROWS), :] = rows[:, :LANES]
                    packed = rows[:, LANES:] if j == 0 else jnp.where(lane_group == j, rows[:, LANES:], packed)
                view[pl.ds(y, lefts, stride=ROWS), :] = packed

    def send_tiles(t, g):
        for k in pieces:
            for o in range(lefts - 1, 0, -1):
                send_tile(t, g, k, o).start()

    def stage1(t, carry):
        for b in range(blocks):
            tile_copy(t, b).wait()

        @pl.when(t + AHEAD < tiles)
        def _():
            for b in range(blocks):
                tile_copy(t + AHEAD, b).start()

        def piece(y):
            values = jnp.concatenate(
                [held.at[t, b].reshape(size_x * ROWS, LANES)[pl.ds(y, size_x, stride=ROWS), :] for b in range(blocks)],
                axis=1)
            both = split(values)
            halves[t, y, 0] = both[0]
            halves[t, y, 1] = both[1]
            return both

        transform(t, 0, 1, piece)

        @pl.when(t == 0)
        def _():
            pl.semaphore_wait(barrier, lefts + rights - 2)
            copy_y.start()
            copy_w.start()

        send_tiles(t, 0)
        return carry

    lax.fori_loop(0, tiles, stage1, 0)
    copy_y.wait()

    def own(g):
        for t in range(tiles):
            for s in range(unit):
                lines[left, t, g * unit + s] = first[t, g, s, left]

    def stage2(g, k):
        at = g * unit + begins[k]
        values = jnp.concatenate(
            [lines[:, :, at + s].reshape(size_y, LANES) for s in range(cuts[k])], axis=1)
        result = product(ty[...], split(values))
        for s in range(cuts[k]):
            second[at + s] = result[:, s * LANES : (s + 1) * LANES]
        for o in range(rights - 1, 0, -1):
            send_right(g, k, o).start()
        for s in range(cuts[k]):
            pencils[right, at + s] = second[at + s, pl.ds(pl.multiple_of(right * share_y, share_y), share_y), :]

    own(0)

    def later1(t, carry):
        transform(t, 1, groups, lambda y: (halves[t, y, 0], halves[t, y, 1]))
        for g in range(1, early):
            send_tiles(t, g)
        for k in pieces:
            @pl.when(t == min(1 + k, tiles - 1))
            def _():
                wait_left(0, k)
                stage2(0, k)
        return carry

    lax.fori_loop(0, tiles, later1, 0)

    def start1(g, carry):
        for k in pieces:
            for o in range(lefts - 1, 0, -1):
                send_left(g, k, o).start()
        return carry

    lax.fori_loop(early, groups, start1, 0)
    copy_w.wait()

    pick = lax.broadcasted_iota(jnp.int32, (share_y, symbol_y.shape[1]), 1) == (
        right * share_y + lax.broadcasted_iota(jnp.int32, (share_y, symbol_y.shape[1]), 0))
    part_y = jnp.sum(jnp.where(pick, symbol_y[...], 0.0), axis=1, keepdims=True)
    modes_z = done.shape[2]
    wide_group = lax.broadcasted_iota(jnp.int32, (share_y, LANES), 1) // rest

    def stage3(g):
        for s in range(group):
            x = g * group + s
            symbol = (symbol_x[left * share_x + x] + part_y) + symbol_z[:, :modes_z]
            done[x] = (1.0 - 0.2 * symbol) / (1.0 + 0.2 * symbol)
        total = None
        for o in range(rights):
            if o > 0:
                wait_right(g, o)
            p = lax.bitwise_xor(right, o)
            main = pencils[p, pl.ds(g * unit + 1, group)].reshape(group * share_y, LANES)
            packed = pencils[p, g * unit]
            other = jnp.concatenate([jnp.where(wide_group == j, packed, 0.0) for j in range(group)], axis=0)
            at = pl.ds(pl.multiple_of(p * 2 * LANES, 2 * LANES), 2 * LANES)
            part = product(stacked(jnp.concatenate([main, other], axis=1)), (tw[0, at, :], tw[1, at, :]))
            total = part if total is None else total + part
        for s in range(group):
            x = g * group + s
            done[x] = total[s * share_y : (s + 1) * share_y] * done[x]
        result_copy(g).start()

    def stage23(g, carry):
        @pl.when(g < groups)
        def _():
            own(g)
            for k in pieces:
                wait_left(g, k)
                stage2(g, k)

        stage3(g - 1)
        return carry

    lax.fori_loop(1, groups + 1, stage23, 0)

    all_left(0, groups * unit, came_left.at[0, 0]).wait_send()
    part = pencils.at[pl.ds(0, rights - 1)]
    pltpu.make_async_remote_copy(
        src_ref=part, dst_ref=part, send_sem=sent_right.at[0], recv_sem=came_right.at[0, 0],
        device_id=(left, lax.bitwise_xor(right, 1)), device_id_type=MESH).wait_send()

    def finish(g, carry):
        result_copy(g).wait()
        return carry

    lax.fori_loop(0, groups, finish, 0)


def body(lefts, rights, signal, symbol_x, symbol_y, symbol_z):
    size_x, own_y, own_z = signal.shape
    size_y, size_z = own_y * lefts, own_z * rights
    modes_x, modes_y, modes_z = size_x // 2, size_y // 2, size_z // 2
    share_x, share_y = modes_x // lefts, modes_y // rights
    blocks, tiles = own_z // LANES, own_y // ROWS
    group = LANES // REST
    groups = share_x // group
    slots = share_x + groups
    cuts = (2, group - 1)
    basis = half_band_basis(own_z, LANES + REST)
    rows_x = kept_table(size_x).T.reshape(lefts, groups, group, size_x).transpose(1, 2, 0, 3)
    rows_x = rows_x.reshape(groups, group * lefts, size_x)
    table_x = np.concatenate(
        [np.concatenate(two_halves(np.concatenate(part))) for part in (rows_x[:1], rows_x[1:])])
    table_y = np.concatenate(two_halves(kept_table(size_y).T))
    table_v = two_halves(np.concatenate([basis[:, :LANES]] + [basis[:, LANES:]] * group, axis=1))
    rows = np.einsum("ic,pik->pck", basis, kept_table(size_z).reshape(rights, own_z, modes_z))
    table_w = two_halves(
        np.concatenate([rows[:, :LANES]] + [rows[:, LANES:]] * group, axis=1).reshape(rights * 2 * LANES, modes_z))
    vmem = pl.BlockSpec(memory_space=pltpu.VMEM)
    hbm = pl.BlockSpec(memory_space=pltpu.HBM)
    smem = pl.BlockSpec(memory_space=pltpu.SMEM)
    dma = pltpu.SemaphoreType.DMA
    return pl.pallas_call(
        functools.partial(kernel, lefts, rights, group, cuts),
        out_shape=jax.ShapeDtypeStruct((share_x, share_y, modes_z), jnp.float32),
        in_specs=[hbm] * 5 + [smem, vmem, vmem],
        out_specs=hbm,
        scratch_shapes=[
            pltpu.VMEM((tiles, blocks, size_x, ROWS, LANES), jnp.float32),
            pltpu.VMEM((tiles, ROWS, 2, size_x, own_z), jnp.bfloat16),
            pltpu.VMEM(table_x.shape, jnp.bfloat16),
            pltpu.VMEM(table_y.shape, jnp.bfloat16),
            pltpu.VMEM(table_v.shape, jnp.bfloat16),
            pltpu.VMEM(table_w.shape, jnp.bfloat16),
            pltpu.VMEM((tiles, groups, group + 1, lefts, ROWS, LANES), jnp.float32),
            pltpu.VMEM((lefts, tiles, slots, ROWS, LANES), jnp.float32),
            pltpu.VMEM((slots, modes_y, LANES), jnp.float32),
            pltpu.VMEM((rights, slots, share_y, LANES), jnp.float32),
            pltpu.VMEM((share_x, share_y, modes_z), jnp.float32),
            dma((tiles, blocks)),
            dma((4,)),
            dma((1,)),
            dma((1,)),
            dma((groups, len(cuts))),
            dma((rights, groups)),
            dma((groups,)),
        ],
        compiler_params=pltpu.CompilerParams(
            collective_id=0, has_side_effects=True, vmem_limit_bytes=62 * 2**20),
    )(signal, table_x, table_y, table_v, table_w, symbol_x, symbol_y[None, :], symbol_z[None, :])


def solution(mesh):
    lefts, rights = mesh.shape["left"], mesh.shape["right"]
    in_specs = (P(None, "left", "right"), P(), P(), P())
    out_specs = P("left", "right", None)
    return jax.shard_map(
        functools.partial(body, lefts, rights), mesh=mesh, in_specs=in_specs, out_specs=out_specs, check_vma=False)
```

```python
import functools

import jax
import jax.numpy as jnp
import numpy as np
from jax import lax
from jax.experimental import pallas as pl
from jax.experimental.pallas import tpu as pltpu
from jax.sharding import PartitionSpec as P

MESH = pl.DeviceIdType.MESH
LANES = 128
ROWS = 8
AHEAD = 2
REST = 32


def kept_table(count):
    rank = np.arange(count)
    odd = 2 * rank + 1
    angle = np.pi / (4 * count) * ((odd[:, None] * odd[None, : count // 2]) % (8 * count))
    return np.cos(angle) * (2.0 / count) ** 0.5


def half_band_basis(count, keep):
    at = np.arange(1, count)
    off = at * (count - at) / 2.0
    columns = np.linalg.eigh(np.diag(off, 1) + np.diag(off, -1))[1][:, ::-1][:, :keep]
    peak = columns[np.abs(columns).argmax(axis=0), np.arange(keep)]
    return columns * np.where(peak < 0, -1.0, 1.0)


def two_halves(table):
    high = table.astype(np.float32).astype(jnp.bfloat16)
    rest = table - high.astype(np.float64)
    return np.stack([high, rest.astype(np.float32).astype(jnp.bfloat16)])


def split(values):
    high = values.astype(jnp.bfloat16)
    return high, (values - high.astype(jnp.float32)).astype(jnp.bfloat16)


def product(first, second):
    dot = functools.partial(jnp.dot, preferred_element_type=jnp.float32)
    rows = first.shape[0] // 2
    both = dot(first, second[0])
    return both[:rows] + (dot(first[:rows], second[1]) + both[rows:])


def stacked(values):
    return jnp.concatenate(split(values), axis=0)


def kernel(
    lefts, rights, group, cuts,
    signal, table_x, table_y, table_v, table_w, symbol_x, symbol_y, symbol_z, out,
    held, halves, tx, ty, tv, tw, first, lines, second, pencils, done,
    held_sem, table_sem, sent_left, sent_right, came_left, came_right, out_sem,
):
    left, right = lax.axis_index("left"), lax.axis_index("right")
    tiles, blocks, size_x = held.shape[0], held.shape[1], held.shape[2]
    groups, unit = first.shape[1], first.shape[2]
    share_x = done.shape[0]
    size_y = lefts * tiles * ROWS
    modes_y = size_y // 2
    share_y = modes_y // rights
    rest = LANES // group
    rows_g = group * lefts
    begins = [sum(cuts[:k]) for k in range(len(cuts))]
    pieces = range(len(cuts))
    lane_group = lax.broadcasted_iota(jnp.int32, (lefts, LANES), 1) // rest

    def tile_copy(t, b):
        return pltpu.make_async_copy(
            signal.at[:, pl.ds(t * ROWS, ROWS), pl.ds(b * LANES, LANES)],
            held.at[t, b], held_sem.at[t, b])

    copy_x = pltpu.make_async_copy(table_x, tx, table_sem.at[0])
    copy_v = pltpu.make_async_copy(table_v, tv, table_sem.at[1])
    copy_y = pltpu.make_async_copy(table_y, ty, table_sem.at[2])
    copy_w = pltpu.make_async_copy(table_w, tw, table_sem.at[3])
    copy_x.start()
    for b in range(blocks):
        tile_copy(0, b).start()
    copy_v.start()

    barrier = pltpu.get_barrier_semaphore()
    for o in range(1, lefts):
        pl.semaphore_signal(barrier, 1, device_id=(lax.bitwise_xor(left, o), right), device_id_type=MESH)
    for o in range(1, rights):
        pl.semaphore_signal(barrier, 1, device_id=(left, lax.bitwise_xor(right, o)), device_id_type=MESH)

    copy_x.wait()
    copy_v.wait()
    for t in range(1, min(AHEAD, tiles)):
        for b in range(blocks):
            tile_copy(t, b).start()

    def send_tile(t, o):
        to = lax.bitwise_xor(left, o)
        return pltpu.make_async_remote_copy(
            src_ref=first.at[t, 0, pl.ds(0, cuts[0]), to],
            dst_ref=lines.at[left, t, pl.ds(0, cuts[0])],
            send_sem=sent_left.at[0], recv_sem=came_left.at[0, 0],
            device_id=(to, right), device_id_type=MESH)

    def send_left(g, k, o):
        to = lax.bitwise_xor(left, o)
        return pltpu.make_async_remote_copy(
            src_ref=first.at[:, g, pl.ds(begins[k], cuts[k]), to],
            dst_ref=lines.at[left, :, pl.ds(g * unit + begins[k], cuts[k])],
            send_sem=sent_left.at[0], recv_sem=came_left.at[g, k],
            device_id=(to, right), device_id_type=MESH)

    def send_right(g, k, o):
        to = lax.bitwise_xor(right, o)
        at = g * unit + begins[k]
        return pltpu.make_async_remote_copy(
            src_ref=second.at[pl.ds(at, cuts[k]), pl.ds(pl.multiple_of(to * share_y, share_y), share_y), :],
            dst_ref=pencils.at[right, pl.ds(at, cuts[k])],
            send_sem=sent_right.at[0], recv_sem=came_right.at[o, g],
            device_id=(left, to), device_id_type=MESH)

    def all_left(k_at, k_count, recv):
        part = lines.at[pl.ds(0, lefts - 1), :, pl.ds(k_at, k_count)]
        return pltpu.make_async_remote_copy(
            src_ref=part, dst_ref=part, send_sem=sent_left.at[0], recv_sem=recv,
            device_id=(lax.bitwise_xor(left, 1), right), device_id_type=MESH)

    def wait_left(g, k):
        all_left(g * unit + begins[k], cuts[k], came_left.at[g, k]).wait_recv()

    def wait_right(g, o):
        part = pencils.at[0, pl.ds(g * unit, unit)]
        pltpu.make_async_remote_copy(
            src_ref=part, dst_ref=part, send_sem=sent_right.at[0], recv_sem=came_right.at[o, g],
            device_id=(left, lax.bitwise_xor(right, o)), device_id_type=MESH).wait_recv()

    def result_copy(g):
        return pltpu.make_async_copy(
            done.at[pl.ds(g * group, group)], out.at[pl.ds(g * group, group)], out_sem.at[g])

    def transform(t, low, high, piece):
        parts = []
        for y in range(ROWS):
            parts.append(product(tx[pl.ds(2 * low * rows_g, 2 * (high - low) * rows_g), :], piece(y)))
        result = product(stacked(jnp.concatenate(parts, axis=0)), (tv[0], tv[1]))
        for y in range(ROWS):
            for g in range(low, high):
                view = first.at[t, g].reshape(unit * lefts * ROWS, LANES)
                packed = None
                for j in range(group):
                    at = ((y * (high - low) + g - low) * group + j) * lefts
                    rows = result[at : at + lefts]
                    view[pl.ds((1 + j) * lefts * ROWS + y, lefts, stride=ROWS), :] = rows[:, :LANES]
                    packed = rows[:, LANES:] if j == 0 else jnp.where(lane_group == j, rows[:, LANES:], packed)
                view[pl.ds(y, lefts, stride=ROWS), :] = packed

    def send_group(g, k):
        for o in range(lefts - 1, 0, -1):
            send_left(g, k, o).start()

    def stage1(t, carry):
        for b in range(blocks):
            tile_copy(t, b).wait()

        @pl.when(t + AHEAD < tiles)
        def _():
            for b in range(blocks):
                tile_copy(t + AHEAD, b).start()

        def piece(y):
            values = jnp.concatenate(
                [held.at[t, b].reshape(size_x * ROWS, LANES)[pl.ds(y, size_x, stride=ROWS), :] for b in range(blocks)],
                axis=1)
            both = split(values)
            halves[t, y, 0] = both[0]
            halves[t, y, 1] = both[1]
            return both

        transform(t, 0, 1, piece)

        @pl.when(t == 0)
        def _():
            pl.semaphore_wait(barrier, lefts + rights - 2)
            copy_y.start()
            copy_w.start()

        for o in range(lefts - 1, 0, -1):
            send_tile(t, o).start()
        return carry

    lax.fori_loop(0, tiles, stage1, 0)
    for k in pieces[1:]:
        send_group(0, k)
    copy_y.wait()

    def own(g):
        for t in range(tiles):
            for s in range(unit):
                lines[left, t, g * unit + s] = first[t, g, s, left]

    def stage2(g, k):
        at = g * unit + begins[k]
        values = jnp.concatenate(
            [lines[:, :, at + s].reshape(size_y, LANES) for s in range(cuts[k])], axis=1)
        result = product(ty[...], split(values))
        for s in range(cuts[k]):
            second[at + s] = result[:, s * LANES : (s + 1) * LANES]
        for o in range(rights - 1, 0, -1):
            send_right(g, k, o).start()
        for s in range(cuts[k]):
            pencils[right, at + s] = second[at + s, pl.ds(pl.multiple_of(right * share_y, share_y), share_y), :]

    own(0)

    def later1(t, carry):
        transform(t, 1, groups, lambda y: (halves[t, y, 0], halves[t, y, 1]))

        @pl.when(t == min(1, tiles - 1))
        def _():
            wait_left(0, 0)
            stage2(0, 0)

        return carry

    lax.fori_loop(0, tiles, later1, 0)

    def start1(g, carry):
        for k in pieces:
            send_group(g, k)
        return carry

    lax.fori_loop(1, groups, start1, 0)
    copy_w.wait()

    pick = lax.broadcasted_iota(jnp.int32, (share_y, symbol_y.shape[1]), 1) == (
        right * share_y + lax.broadcasted_iota(jnp.int32, (share_y, symbol_y.shape[1]), 0))
    part_y = jnp.sum(jnp.where(pick, symbol_y[...], 0.0), axis=1, keepdims=True)
    modes_z = done.shape[2]
    wide_group = lax.broadcasted_iota(jnp.int32, (share_y, LANES), 1) // rest

    def stage3(g):
        for s in range(group):
            x = g * group + s
            symbol = (symbol_x[left * share_x + x] + part_y) + symbol_z[:, :modes_z]
            done[x] = (1.0 - 0.2 * symbol) / (1.0 + 0.2 * symbol)
        total = None
        for o in range(rights):
            if o > 0:
                wait_right(g, o)
            p = lax.bitwise_xor(right, o)
            main = pencils[p, pl.ds(g * unit + 1, group)].reshape(group * share_y, LANES)
            packed = pencils[p, g * unit]
            other = jnp.concatenate([jnp.where(wide_group == j, packed, 0.0) for j in range(group)], axis=0)
            at = pl.ds(pl.multiple_of(p * 2 * LANES, 2 * LANES), 2 * LANES)
            part = product(stacked(jnp.concatenate([main, other], axis=1)), (tw[0, at, :], tw[1, at, :]))
            total = part if total is None else total + part
        for s in range(group):
            x = g * group + s
            done[x] = total[s * share_y : (s + 1) * share_y] * done[x]
        result_copy(g).start()

    def stage23(g, carry):
        @pl.when(g < groups)
        def _():
            @pl.when(g > 0)
            def _():
                own(g)
                wait_left(g, 0)
                stage2(g, 0)

            for k in pieces[1:]:
                wait_left(g, k)
                stage2(g, k)

        @pl.when(g > 0)
        def _():
            stage3(g - 1)

        return carry

    lax.fori_loop(0, groups + 1, stage23, 0)

    all_left(0, groups * unit, came_left.at[0, 0]).wait_send()
    part = pencils.at[pl.ds(0, rights - 1)]
    pltpu.make_async_remote_copy(
        src_ref=part, dst_ref=part, send_sem=sent_right.at[0], recv_sem=came_right.at[0, 0],
        device_id=(left, lax.bitwise_xor(right, 1)), device_id_type=MESH).wait_send()

    def finish(g, carry):
        result_copy(g).wait()
        return carry

    lax.fori_loop(0, groups, finish, 0)


def body(lefts, rights, signal, symbol_x, symbol_y, symbol_z):
    size_x, own_y, own_z = signal.shape
    size_y, size_z = own_y * lefts, own_z * rights
    modes_x, modes_y, modes_z = size_x // 2, size_y // 2, size_z // 2
    share_x, share_y = modes_x // lefts, modes_y // rights
    blocks, tiles = own_z // LANES, own_y // ROWS
    group = LANES // REST
    groups = share_x // group
    slots = share_x + groups
    cuts = (2, 2, 1)
    basis = half_band_basis(own_z, LANES + REST)
    rows_x = kept_table(size_x).T.reshape(lefts, groups, group, size_x).transpose(1, 2, 0, 3)
    rows_x = rows_x.reshape(groups, group * lefts, size_x)
    table_x = np.concatenate(
        [np.concatenate(two_halves(np.concatenate(part))) for part in (rows_x[:1], rows_x[1:])])
    table_y = np.concatenate(two_halves(kept_table(size_y).T))
    table_v = two_halves(np.concatenate([basis[:, :LANES]] + [basis[:, LANES:]] * group, axis=1))
    rows = np.einsum("ic,pik->pck", basis, kept_table(size_z).reshape(rights, own_z, modes_z))
    table_w = two_halves(
        np.concatenate([rows[:, :LANES]] + [rows[:, LANES:]] * group, axis=1).reshape(rights * 2 * LANES, modes_z))
    vmem = pl.BlockSpec(memory_space=pltpu.VMEM)
    hbm = pl.BlockSpec(memory_space=pltpu.HBM)
    smem = pl.BlockSpec(memory_space=pltpu.SMEM)
    dma = pltpu.SemaphoreType.DMA
    return pl.pallas_call(
        functools.partial(kernel, lefts, rights, group, cuts),
        out_shape=jax.ShapeDtypeStruct((share_x, share_y, modes_z), jnp.float32),
        in_specs=[hbm] * 5 + [smem, vmem, vmem],
        out_specs=hbm,
        scratch_shapes=[
            pltpu.VMEM((tiles, blocks, size_x, ROWS, LANES), jnp.float32),
            pltpu.VMEM((tiles, ROWS, 2, size_x, own_z), jnp.bfloat16),
            pltpu.VMEM(table_x.shape, jnp.bfloat16),
            pltpu.VMEM(table_y.shape, jnp.bfloat16),
            pltpu.VMEM(table_v.shape, jnp.bfloat16),
            pltpu.VMEM(table_w.shape, jnp.bfloat16),
            pltpu.VMEM((tiles, groups, group + 1, lefts, ROWS, LANES), jnp.float32),
            pltpu.VMEM((lefts, tiles, slots, ROWS, LANES), jnp.float32),
            pltpu.VMEM((slots, modes_y, LANES), jnp.float32),
            pltpu.VMEM((rights, slots, share_y, LANES), jnp.float32),
            pltpu.VMEM((share_x, share_y, modes_z), jnp.float32),
            dma((tiles, blocks)),
            dma((4,)),
            dma((1,)),
            dma((1,)),
            dma((groups, len(cuts))),
            dma((rights, groups)),
            dma((groups,)),
        ],
        compiler_params=pltpu.CompilerParams(
            collective_id=0, has_side_effects=True, vmem_limit_bytes=62 * 2**20),
    )(signal, table_x, table_y, table_v, table_w, symbol_x, symbol_y[None, :], symbol_z[None, :])


def solution(mesh):
    lefts, rights = mesh.shape["left"], mesh.shape["right"]
    in_specs = (P(None, "left", "right"), P(), P(), P())
    out_specs = P("left", "right", None)
    return jax.shard_map(
        functools.partial(body, lefts, rights), mesh=mesh, in_specs=in_specs, out_specs=out_specs, check_vma=False)
```

```python
import functools

import jax
import jax.numpy as jnp
import numpy as np
from jax import lax
from jax.experimental import pallas as pl
from jax.experimental.pallas import tpu as pltpu
from jax.sharding import PartitionSpec as P

MESH = pl.DeviceIdType.MESH
LANES = 128
ROWS = 8
AHEAD = 2
TILED = (1, 1)
REST = 32


def kept_table(count):
    rank = np.arange(count)
    odd = 2 * rank + 1
    angle = np.pi / (4 * count) * ((odd[:, None] * odd[None, : count // 2]) % (8 * count))
    return np.cos(angle) * (2.0 / count) ** 0.5


def half_band_basis(count, keep):
    at = np.arange(1, count)
    off = at * (count - at) / 2.0
    columns = np.linalg.eigh(np.diag(off, 1) + np.diag(off, -1))[1][:, ::-1][:, :keep]
    peak = columns[np.abs(columns).argmax(axis=0), np.arange(keep)]
    return columns * np.where(peak < 0, -1.0, 1.0)


def two_halves(table):
    high = table.astype(np.float32).astype(jnp.bfloat16)
    rest = table - high.astype(np.float64)
    return np.stack([high, rest.astype(np.float32).astype(jnp.bfloat16)])


def split(values):
    high = values.astype(jnp.bfloat16)
    return high, (values - high.astype(jnp.float32)).astype(jnp.bfloat16)


def product(first, second):
    dot = functools.partial(jnp.dot, preferred_element_type=jnp.float32)
    rows = first.shape[0] // 2
    both = dot(first, second[0])
    return both[:rows] + (dot(first[:rows], second[1]) + both[rows:])


def stacked(values):
    return jnp.concatenate(split(values), axis=0)


def kernel(
    lefts, rights, group, cuts,
    signal, table_x, table_y, table_v, table_w, symbol_x, symbol_y, symbol_z, out,
    held, halves, tx, ty, tv, tw, first, lines, second, pencils, done,
    held_sem, table_sem, sent_left, sent_right, came_left, came_right, out_sem,
):
    left, right = lax.axis_index("left"), lax.axis_index("right")
    tiles, blocks, size_x = held.shape[0], held.shape[1], held.shape[2]
    groups, unit = first.shape[1], first.shape[2]
    share_x = done.shape[0]
    size_y = lefts * tiles * ROWS
    modes_y = size_y // 2
    share_y = modes_y // rights
    rest = LANES // group
    rows_g = group * lefts
    begins = [sum(cuts[:k]) for k in range(len(cuts))]
    pieces = range(len(cuts))
    lane_group = lax.broadcasted_iota(jnp.int32, (lefts, LANES), 1) // rest

    def tile_copy(t, b):
        return pltpu.make_async_copy(
            signal.at[:, pl.ds(t * ROWS, ROWS), pl.ds(b * LANES, LANES)],
            held.at[t, b], held_sem.at[t, b])

    copy_x = pltpu.make_async_copy(table_x, tx, table_sem.at[0])
    copy_v = pltpu.make_async_copy(table_v, tv, table_sem.at[1])
    copy_y = pltpu.make_async_copy(table_y, ty, table_sem.at[2])
    copy_w = pltpu.make_async_copy(table_w, tw, table_sem.at[3])
    copy_x.start()
    for b in range(blocks):
        tile_copy(0, b).start()
    copy_v.start()

    barrier = pltpu.get_barrier_semaphore()
    for o in range(1, lefts):
        pl.semaphore_signal(barrier, 1, device_id=(lax.bitwise_xor(left, o), right), device_id_type=MESH)
    for o in range(1, rights):
        pl.semaphore_signal(barrier, 1, device_id=(left, lax.bitwise_xor(right, o)), device_id_type=MESH)

    copy_x.wait()
    copy_v.wait()
    for t in range(1, min(AHEAD, tiles)):
        for b in range(blocks):
            tile_copy(t, b).start()

    def send_tile(t, g, k, o):
        to = lax.bitwise_xor(left, o)
        return pltpu.make_async_remote_copy(
            src_ref=first.at[t, g, pl.ds(begins[k], cuts[k]), to],
            dst_ref=lines.at[left, t, pl.ds(g * unit + begins[k], cuts[k])],
            send_sem=sent_left.at[0], recv_sem=came_left.at[g, k],
            device_id=(to, right), device_id_type=MESH)

    def send_tiles(t, g):
        for k in pieces[: TILED[g]]:
            for o in range(lefts - 1, 0, -1):
                send_tile(t, g, k, o).start()

    def send_left(g, k, o):
        to = lax.bitwise_xor(left, o)
        return pltpu.make_async_remote_copy(
            src_ref=first.at[:, g, pl.ds(begins[k], cuts[k]), to],
            dst_ref=lines.at[left, :, pl.ds(g * unit + begins[k], cuts[k])],
            send_sem=sent_left.at[0], recv_sem=came_left.at[g, k],
            device_id=(to, right), device_id_type=MESH)

    def send_right(g, k, o):
        to = lax.bitwise_xor(right, o)
        at = g * unit + begins[k]
        return pltpu.make_async_remote_copy(
            src_ref=second.at[pl.ds(at, cuts[k]), pl.ds(pl.multiple_of(to * share_y, share_y), share_y), :],
            dst_ref=pencils.at[right, pl.ds(at, cuts[k])],
            send_sem=sent_right.at[0], recv_sem=came_right.at[o, g],
            device_id=(left, to), device_id_type=MESH)

    def all_left(k_at, k_count, recv):
        part = lines.at[pl.ds(0, lefts - 1), :, pl.ds(k_at, k_count)]
        return pltpu.make_async_remote_copy(
            src_ref=part, dst_ref=part, send_sem=sent_left.at[0], recv_sem=recv,
            device_id=(lax.bitwise_xor(left, 1), right), device_id_type=MESH)

    def wait_left(g, k):
        all_left(g * unit + begins[k], cuts[k], came_left.at[g, k]).wait_recv()

    def wait_right(g, o):
        part = pencils.at[0, pl.ds(g * unit, unit)]
        pltpu.make_async_remote_copy(
            src_ref=part, dst_ref=part, send_sem=sent_right.at[0], recv_sem=came_right.at[o, g],
            device_id=(left, lax.bitwise_xor(right, o)), device_id_type=MESH).wait_recv()

    def result_copy(g):
        return pltpu.make_async_copy(
            done.at[pl.ds(g * group, group)], out.at[pl.ds(g * group, group)], out_sem.at[g])

    def transform(t, low, high, piece):
        parts = []
        for y in range(ROWS):
            parts.append(product(tx[pl.ds(2 * low * rows_g, 2 * (high - low) * rows_g), :], piece(y)))
        result = product(stacked(jnp.concatenate(parts, axis=0)), (tv[0], tv[1]))
        for y in range(ROWS):
            for g in range(low, high):
                view = first.at[t, g].reshape(unit * lefts * ROWS, LANES)
                packed = None
                for j in range(group):
                    at = ((y * (high - low) + g - low) * group + j) * lefts
                    rows = result[at : at + lefts]
                    view[pl.ds((1 + j) * lefts * ROWS + y, lefts, stride=ROWS), :] = rows[:, :LANES]
                    packed = rows[:, LANES:] if j == 0 else jnp.where(lane_group == j, rows[:, LANES:], packed)
                view[pl.ds(y, lefts, stride=ROWS), :] = packed

    def send_group(g, k):
        for o in range(lefts - 1, 0, -1):
            send_left(g, k, o).start()

    def stage1(t, carry):
        for b in range(blocks):
            tile_copy(t, b).wait()

        @pl.when(t + AHEAD < tiles)
        def _():
            for b in range(blocks):
                tile_copy(t + AHEAD, b).start()

        def piece(y):
            values = jnp.concatenate(
                [held.at[t, b].reshape(size_x * ROWS, LANES)[pl.ds(y, size_x, stride=ROWS), :] for b in range(blocks)],
                axis=1)
            both = split(values)
            halves[t, y, 0] = both[0]
            halves[t, y, 1] = both[1]
            return both

        transform(t, 0, 1, piece)

        @pl.when(t == 0)
        def _():
            pl.semaphore_wait(barrier, lefts + rights - 2)
            copy_y.start()
            copy_w.start()

        send_tiles(t, 0)
        return carry

    lax.fori_loop(0, tiles, stage1, 0)
    for k in pieces[TILED[0] :]:
        send_group(0, k)
    copy_y.wait()

    def own(g):
        for t in range(tiles):
            for s in range(unit):
                lines[left, t, g * unit + s] = first[t, g, s, left]

    def stage2(g, k):
        at = g * unit + begins[k]
        values = jnp.concatenate(
            [lines[:, :, at + s].reshape(size_y, LANES) for s in range(cuts[k])], axis=1)
        result = product(ty[...], split(values))
        for s in range(cuts[k]):
            second[at + s] = result[:, s * LANES : (s + 1) * LANES]
        for o in sorted(range(1, rights), key=lambda o: (o == 1, o)):
            send_right(g, k, o).start()
        for s in range(cuts[k]):
            pencils[right, at + s] = second[at + s, pl.ds(pl.multiple_of(right * share_y, share_y), share_y), :]

    own(0)

    def later1(t, carry):
        transform(t, 1, groups, lambda y: (halves[t, y, 0], halves[t, y, 1]))
        if groups > 1:
            send_tiles(t, 1)

        @pl.when(t == min(1, tiles - 1))
        def _():
            wait_left(0, 0)
            stage2(0, 0)

        return carry

    lax.fori_loop(0, tiles, later1, 0)

    def start1(g, carry):
        for k in pieces:
            send_group(g, k)
        return carry

    if groups > 1:
        for k in pieces[TILED[1] :]:
            send_group(1, k)
    lax.fori_loop(2, groups, start1, 0)
    copy_w.wait()

    pick = lax.broadcasted_iota(jnp.int32, (share_y, symbol_y.shape[1]), 1) == (
        right * share_y + lax.broadcasted_iota(jnp.int32, (share_y, symbol_y.shape[1]), 0))
    part_y = jnp.sum(jnp.where(pick, symbol_y[...], 0.0), axis=1, keepdims=True)
    modes_z = done.shape[2]
    wide_group = lax.broadcasted_iota(jnp.int32, (share_y, LANES), 1) // rest

    def stage3(g):
        for s in range(group):
            x = g * group + s
            symbol = (symbol_x[left * share_x + x] + part_y) + symbol_z[:, :modes_z]
            done[x] = (1.0 - 0.2 * symbol) / (1.0 + 0.2 * symbol)
        total = None
        for o in range(rights):
            if o > 0:
                wait_right(g, o)
            p = lax.bitwise_xor(right, o)
            main = pencils[p, pl.ds(g * unit + 1, group)].reshape(group * share_y, LANES)
            packed = pencils[p, g * unit]
            other = jnp.concatenate([jnp.where(wide_group == j, packed, 0.0) for j in range(group)], axis=0)
            at = pl.ds(pl.multiple_of(p * 2 * LANES, 2 * LANES), 2 * LANES)
            part = product(stacked(jnp.concatenate([main, other], axis=1)), (tw[0, at, :], tw[1, at, :]))
            total = part if total is None else total + part
        for s in range(group):
            x = g * group + s
            done[x] = total[s * share_y : (s + 1) * share_y] * done[x]
        result_copy(g).start()

    def stage23(g, carry):
        @pl.when(g < groups)
        def _():
            @pl.when(g > 0)
            def _():
                own(g)
                wait_left(g, 0)
                stage2(g, 0)

            for k in pieces[1:]:
                wait_left(g, k)
                stage2(g, k)

        @pl.when(g > 0)
        def _():
            stage3(g - 1)

        return carry

    lax.fori_loop(0, groups + 1, stage23, 0)

    all_left(0, groups * unit, came_left.at[0, 0]).wait_send()
    part = pencils.at[pl.ds(0, rights - 1)]
    pltpu.make_async_remote_copy(
        src_ref=part, dst_ref=part, send_sem=sent_right.at[0], recv_sem=came_right.at[0, 0],
        device_id=(left, lax.bitwise_xor(right, 1)), device_id_type=MESH).wait_send()

    def finish(g, carry):
        result_copy(g).wait()
        return carry

    lax.fori_loop(0, groups, finish, 0)


def body(lefts, rights, signal, symbol_x, symbol_y, symbol_z):
    size_x, own_y, own_z = signal.shape
    size_y, size_z = own_y * lefts, own_z * rights
    modes_x, modes_y, modes_z = size_x // 2, size_y // 2, size_z // 2
    share_x, share_y = modes_x // lefts, modes_y // rights
    blocks, tiles = own_z // LANES, own_y // ROWS
    group = LANES // REST
    groups = share_x // group
    slots = share_x + groups
    cuts = (2, 1, 1, 1)
    basis = half_band_basis(own_z, LANES + REST)
    rows_x = kept_table(size_x).T.reshape(lefts, groups, group, size_x).transpose(1, 2, 0, 3)
    rows_x = rows_x.reshape(groups, group * lefts, size_x)
    table_x = np.concatenate(
        [np.concatenate(two_halves(np.concatenate(part))) for part in (rows_x[:1], rows_x[1:])])
    table_y = np.concatenate(two_halves(kept_table(size_y).T))
    table_v = two_halves(np.concatenate([basis[:, :LANES]] + [basis[:, LANES:]] * group, axis=1))
    rows = np.einsum("ic,pik->pck", basis, kept_table(size_z).reshape(rights, own_z, modes_z))
    table_w = two_halves(
        np.concatenate([rows[:, :LANES]] + [rows[:, LANES:]] * group, axis=1).reshape(rights * 2 * LANES, modes_z))
    vmem = pl.BlockSpec(memory_space=pltpu.VMEM)
    hbm = pl.BlockSpec(memory_space=pltpu.HBM)
    smem = pl.BlockSpec(memory_space=pltpu.SMEM)
    dma = pltpu.SemaphoreType.DMA
    return pl.pallas_call(
        functools.partial(kernel, lefts, rights, group, cuts),
        out_shape=jax.ShapeDtypeStruct((share_x, share_y, modes_z), jnp.float32),
        in_specs=[hbm] * 5 + [smem, vmem, vmem],
        out_specs=hbm,
        scratch_shapes=[
            pltpu.VMEM((tiles, blocks, size_x, ROWS, LANES), jnp.float32),
            pltpu.VMEM((tiles, ROWS, 2, size_x, own_z), jnp.bfloat16),
            pltpu.VMEM(table_x.shape, jnp.bfloat16),
            pltpu.VMEM(table_y.shape, jnp.bfloat16),
            pltpu.VMEM(table_v.shape, jnp.bfloat16),
            pltpu.VMEM(table_w.shape, jnp.bfloat16),
            pltpu.VMEM((tiles, groups, group + 1, lefts, ROWS, LANES), jnp.float32),
            pltpu.VMEM((lefts, tiles, slots, ROWS, LANES), jnp.float32),
            pltpu.VMEM((slots, modes_y, LANES), jnp.float32),
            pltpu.VMEM((rights, slots, share_y, LANES), jnp.float32),
            pltpu.VMEM((share_x, share_y, modes_z), jnp.float32),
            dma((tiles, blocks)),
            dma((4,)),
            dma((1,)),
            dma((1,)),
            dma((groups, len(cuts))),
            dma((rights, groups)),
            dma((groups,)),
        ],
        compiler_params=pltpu.CompilerParams(
            collective_id=0, has_side_effects=True, vmem_limit_bytes=62 * 2**20),
    )(signal, table_x, table_y, table_v, table_w, symbol_x, symbol_y[None, :], symbol_z[None, :])


def solution(mesh):
    lefts, rights = mesh.shape["left"], mesh.shape["right"]
    in_specs = (P(None, "left", "right"), P(), P(), P())
    out_specs = P("left", "right", None)
    return jax.shard_map(
        functools.partial(body, lefts, rights), mesh=mesh, in_specs=in_specs, out_specs=out_specs, check_vma=False)
```

```python
import functools

import jax
import jax.numpy as jnp
import numpy as np
from jax import lax
from jax.experimental import pallas as pl
from jax.experimental.pallas import tpu as pltpu
from jax.sharding import PartitionSpec as P

MESH = pl.DeviceIdType.MESH
LANES = 128
ROWS = 8
AHEAD = 2
TILED = (1, 1)
REST = 32


def kept_table(count):
    rank = np.arange(count)
    odd = 2 * rank + 1
    angle = np.pi / (4 * count) * ((odd[:, None] * odd[None, : count // 2]) % (8 * count))
    return np.cos(angle) * (2.0 / count) ** 0.5


def half_band_basis(count, keep):
    at = np.arange(1, count)
    off = at * (count - at) / 2.0
    columns = np.linalg.eigh(np.diag(off, 1) + np.diag(off, -1))[1][:, ::-1][:, :keep]
    peak = columns[np.abs(columns).argmax(axis=0), np.arange(keep)]
    return columns * np.where(peak < 0, -1.0, 1.0)


def two_halves(table):
    high = table.astype(np.float32).astype(jnp.bfloat16)
    rest = table - high.astype(np.float64)
    return np.stack([high, rest.astype(np.float32).astype(jnp.bfloat16)])


def split(values):
    high = values.astype(jnp.bfloat16)
    return high, (values - high.astype(jnp.float32)).astype(jnp.bfloat16)


def product(first, second):
    dot = functools.partial(jnp.dot, preferred_element_type=jnp.float32)
    rows = first.shape[0] // 2
    both = dot(first, second[0])
    return both[:rows] + (dot(first[:rows], second[1]) + both[rows:])


def stacked(values):
    return jnp.concatenate(split(values), axis=0)


def kernel(
    lefts, rights, group, cuts,
    signal, table_x, table_y, table_v, table_w, symbol_x, symbol_y, symbol_z, out,
    held, halves, tx, ty, tv, tw, first, lines, second, pencils, done,
    held_sem, table_sem, sent_left, sent_right, came_left, came_right, out_sem,
):
    left, right = lax.axis_index("left"), lax.axis_index("right")
    tiles, blocks, size_x = held.shape[0], held.shape[1], held.shape[2]
    groups, unit = first.shape[1], first.shape[3]
    share_x = done.shape[0]
    size_y = lefts * tiles * ROWS
    modes_y = size_y // 2
    share_y = modes_y // rights
    rest = LANES // group
    rows_g = group * lefts
    begins = [sum(cuts[:k]) for k in range(len(cuts))]
    pieces = range(len(cuts))
    lane_group = lax.broadcasted_iota(jnp.int32, (lefts, LANES), 1) // rest

    def tile_copy(t, b):
        return pltpu.make_async_copy(
            signal.at[:, pl.ds(t * ROWS, ROWS), pl.ds(b * LANES, LANES)],
            held.at[t, b], held_sem.at[t, b])

    copy_x = pltpu.make_async_copy(table_x, tx, table_sem.at[0])
    copy_v = pltpu.make_async_copy(table_v, tv, table_sem.at[1])
    copy_y = pltpu.make_async_copy(table_y, ty, table_sem.at[2])
    copy_w = pltpu.make_async_copy(table_w, tw, table_sem.at[3])
    copy_x.start()
    for b in range(blocks):
        tile_copy(0, b).start()
    copy_v.start()

    barrier = pltpu.get_barrier_semaphore()
    for o in range(1, lefts):
        pl.semaphore_signal(barrier, 1, device_id=(lax.bitwise_xor(left, o), right), device_id_type=MESH)
    for o in range(1, rights):
        pl.semaphore_signal(barrier, 1, device_id=(left, lax.bitwise_xor(right, o)), device_id_type=MESH)

    copy_x.wait()
    copy_v.wait()
    for t in range(1, min(AHEAD, tiles)):
        for b in range(blocks):
            tile_copy(t, b).start()

    def send_tile(t, g, k, o):
        to = lax.bitwise_xor(left, o)
        return pltpu.make_async_remote_copy(
            src_ref=first.at[t, g, to, pl.ds(begins[k], cuts[k])],
            dst_ref=lines.at[left, t, pl.ds(g * unit + begins[k], cuts[k])],
            send_sem=sent_left.at[0], recv_sem=came_left.at[g, k],
            device_id=(to, right), device_id_type=MESH)

    def send_tiles(t, g):
        for k in pieces[: TILED[g]]:
            for o in range(lefts - 1, 0, -1):
                send_tile(t, g, k, o).start()

    def send_left(g, k, o):
        to = lax.bitwise_xor(left, o)
        return pltpu.make_async_remote_copy(
            src_ref=first.at[:, g, to, pl.ds(begins[k], cuts[k])],
            dst_ref=lines.at[left, :, pl.ds(g * unit + begins[k], cuts[k])],
            send_sem=sent_left.at[0], recv_sem=came_left.at[g, k],
            device_id=(to, right), device_id_type=MESH)

    def send_right(g, k, o):
        to = lax.bitwise_xor(right, o)
        at = g * unit + begins[k]
        return pltpu.make_async_remote_copy(
            src_ref=second.at[pl.ds(at, cuts[k]), pl.ds(pl.multiple_of(to * share_y, share_y), share_y), :],
            dst_ref=pencils.at[right, pl.ds(at, cuts[k])],
            send_sem=sent_right.at[0], recv_sem=came_right.at[o, g],
            device_id=(left, to), device_id_type=MESH)

    def all_left(k_at, k_count, recv):
        part = lines.at[pl.ds(0, lefts - 1), :, pl.ds(k_at, k_count)]
        return pltpu.make_async_remote_copy(
            src_ref=part, dst_ref=part, send_sem=sent_left.at[0], recv_sem=recv,
            device_id=(lax.bitwise_xor(left, 1), right), device_id_type=MESH)

    def wait_left(g, k):
        all_left(g * unit + begins[k], cuts[k], came_left.at[g, k]).wait_recv()

    def wait_right(g, o):
        part = pencils.at[0, pl.ds(g * unit, unit)]
        pltpu.make_async_remote_copy(
            src_ref=part, dst_ref=part, send_sem=sent_right.at[0], recv_sem=came_right.at[o, g],
            device_id=(left, lax.bitwise_xor(right, o)), device_id_type=MESH).wait_recv()

    def result_copy(g):
        return pltpu.make_async_copy(
            done.at[pl.ds(g * group, group)], out.at[pl.ds(g * group, group)], out_sem.at[g])

    def transform(t, low, high, piece):
        parts = []
        for y in range(ROWS):
            parts.append(product(tx[pl.ds(2 * low * rows_g, 2 * (high - low) * rows_g), :], piece(y)))
        result = product(stacked(jnp.concatenate(parts, axis=0)), (tv[0], tv[1]))
        for y in range(ROWS):
            for g in range(low, high):
                view = first.at[t, g].reshape(unit * lefts * ROWS, LANES)
                packed = None
                for j in range(group):
                    at = ((y * (high - low) + g - low) * group + j) * lefts
                    rows = result[at : at + lefts]
                    view[pl.ds((1 + j) * ROWS + y, lefts, stride=unit * ROWS), :] = rows[:, :LANES]
                    packed = rows[:, LANES:] if j == 0 else jnp.where(lane_group == j, rows[:, LANES:], packed)
                view[pl.ds(y, lefts, stride=unit * ROWS), :] = packed

    def send_group(g, k):
        for o in range(lefts - 1, 0, -1):
            send_left(g, k, o).start()

    def stage1(t, carry):
        for b in range(blocks):
            tile_copy(t, b).wait()

        @pl.when(t + AHEAD < tiles)
        def _():
            for b in range(blocks):
                tile_copy(t + AHEAD, b).start()

        def piece(y):
            values = jnp.concatenate(
                [held.at[t, b].reshape(size_x * ROWS, LANES)[pl.ds(y, size_x, stride=ROWS), :] for b in range(blocks)],
                axis=1)
            both = split(values)
            halves[t, y, 0] = both[0]
            halves[t, y, 1] = both[1]
            return both

        transform(t, 0, 1, piece)

        @pl.when(t == 0)
        def _():
            pl.semaphore_wait(barrier, lefts + rights - 2)
            copy_y.start()
            copy_w.start()

        send_tiles(t, 0)
        return carry

    lax.fori_loop(0, tiles, stage1, 0)
    for k in pieces[TILED[0] :]:
        send_group(0, k)
    copy_y.wait()

    def own(g):
        for t in range(tiles):
            for s in range(unit):
                lines[left, t, g * unit + s] = first[t, g, left, s]

    def stage2(g, k):
        at = g * unit + begins[k]
        values = jnp.concatenate(
            [lines[:, :, at + s].reshape(size_y, LANES) for s in range(cuts[k])], axis=1)
        result = product(ty[...], split(values))
        for s in range(cuts[k]):
            second[at + s] = result[:, s * LANES : (s + 1) * LANES]
        for o in sorted(range(1, rights), key=lambda o: (o == 1, o)):
            send_right(g, k, o).start()
        for s in range(cuts[k]):
            pencils[right, at + s] = second[at + s, pl.ds(pl.multiple_of(right * share_y, share_y), share_y), :]

    own(0)

    def later1(t, carry):
        transform(t, 1, groups, lambda y: (halves[t, y, 0], halves[t, y, 1]))
        if groups > 1:
            send_tiles(t, 1)

        @pl.when(t == min(1, tiles - 1))
        def _():
            wait_left(0, 0)
            stage2(0, 0)

        return carry

    lax.fori_loop(0, tiles, later1, 0)

    def start1(g, carry):
        for k in pieces:
            send_group(g, k)
        return carry

    if groups > 1:
        for k in pieces[TILED[1] :]:
            send_group(1, k)
    lax.fori_loop(2, groups, start1, 0)
    copy_w.wait()

    pick = lax.broadcasted_iota(jnp.int32, (share_y, symbol_y.shape[1]), 1) == (
        right * share_y + lax.broadcasted_iota(jnp.int32, (share_y, symbol_y.shape[1]), 0))
    part_y = jnp.sum(jnp.where(pick, symbol_y[...], 0.0), axis=1, keepdims=True)
    modes_z = done.shape[2]
    wide_group = lax.broadcasted_iota(jnp.int32, (share_y, LANES), 1) // rest

    def stage3(g):
        for s in range(group):
            x = g * group + s
            symbol = (symbol_x[left * share_x + x] + part_y) + symbol_z[:, :modes_z]
            done[x] = (1.0 - 0.2 * symbol) / (1.0 + 0.2 * symbol)
        total = None
        for o in range(rights):
            if o > 0:
                wait_right(g, o)
            p = lax.bitwise_xor(right, o)
            main = pencils[p, pl.ds(g * unit + 1, group)].reshape(group * share_y, LANES)
            packed = pencils[p, g * unit]
            other = jnp.concatenate([jnp.where(wide_group == j, packed, 0.0) for j in range(group)], axis=0)
            at = pl.ds(pl.multiple_of(p * 2 * LANES, 2 * LANES), 2 * LANES)
            part = product(stacked(jnp.concatenate([main, other], axis=1)), (tw[0, at, :], tw[1, at, :]))
            total = part if total is None else total + part
        for s in range(group):
            x = g * group + s
            done[x] = total[s * share_y : (s + 1) * share_y] * done[x]
        result_copy(g).start()

    def stage23(g, carry):
        @pl.when(g < groups)
        def _():
            @pl.when(g > 0)
            def _():
                own(g)
                wait_left(g, 0)
                stage2(g, 0)

            for k in pieces[1:]:
                wait_left(g, k)
                stage2(g, k)

        @pl.when(g > 0)
        def _():
            stage3(g - 1)

        return carry

    lax.fori_loop(0, groups + 1, stage23, 0)

    all_left(0, groups * unit, came_left.at[0, 0]).wait_send()
    part = pencils.at[pl.ds(0, rights - 1)]
    pltpu.make_async_remote_copy(
        src_ref=part, dst_ref=part, send_sem=sent_right.at[0], recv_sem=came_right.at[0, 0],
        device_id=(left, lax.bitwise_xor(right, 1)), device_id_type=MESH).wait_send()

    def finish(g, carry):
        result_copy(g).wait()
        return carry

    lax.fori_loop(0, groups, finish, 0)


def body(lefts, rights, signal, symbol_x, symbol_y, symbol_z):
    size_x, own_y, own_z = signal.shape
    size_y, size_z = own_y * lefts, own_z * rights
    modes_x, modes_y, modes_z = size_x // 2, size_y // 2, size_z // 2
    share_x, share_y = modes_x // lefts, modes_y // rights
    blocks, tiles = own_z // LANES, own_y // ROWS
    group = LANES // REST
    groups = share_x // group
    slots = share_x + groups
    cuts = (2, 1, 1, 1)
    basis = half_band_basis(own_z, LANES + REST)
    rows_x = kept_table(size_x).T.reshape(lefts, groups, group, size_x).transpose(1, 2, 0, 3)
    rows_x = rows_x.reshape(groups, group * lefts, size_x)
    table_x = np.concatenate(
        [np.concatenate(two_halves(np.concatenate(part))) for part in (rows_x[:1], rows_x[1:])])
    table_y = np.concatenate(two_halves(kept_table(size_y).T))
    table_v = two_halves(np.concatenate([basis[:, :LANES]] + [basis[:, LANES:]] * group, axis=1))
    rows = np.einsum("ic,pik->pck", basis, kept_table(size_z).reshape(rights, own_z, modes_z))
    table_w = two_halves(
        np.concatenate([rows[:, :LANES]] + [rows[:, LANES:]] * group, axis=1).reshape(rights * 2 * LANES, modes_z))
    vmem = pl.BlockSpec(memory_space=pltpu.VMEM)
    hbm = pl.BlockSpec(memory_space=pltpu.HBM)
    smem = pl.BlockSpec(memory_space=pltpu.SMEM)
    dma = pltpu.SemaphoreType.DMA
    return pl.pallas_call(
        functools.partial(kernel, lefts, rights, group, cuts),
        out_shape=jax.ShapeDtypeStruct((share_x, share_y, modes_z), jnp.float32),
        in_specs=[hbm] * 5 + [smem, vmem, vmem],
        out_specs=hbm,
        scratch_shapes=[
            pltpu.VMEM((tiles, blocks, size_x, ROWS, LANES), jnp.float32),
            pltpu.VMEM((tiles, ROWS, 2, size_x, own_z), jnp.bfloat16),
            pltpu.VMEM(table_x.shape, jnp.bfloat16),
            pltpu.VMEM(table_y.shape, jnp.bfloat16),
            pltpu.VMEM(table_v.shape, jnp.bfloat16),
            pltpu.VMEM(table_w.shape, jnp.bfloat16),
            pltpu.VMEM((tiles, groups, lefts, group + 1, ROWS, LANES), jnp.float32),
            pltpu.VMEM((lefts, tiles, slots, ROWS, LANES), jnp.float32),
            pltpu.VMEM((slots, modes_y, LANES), jnp.float32),
            pltpu.VMEM((rights, slots, share_y, LANES), jnp.float32),
            pltpu.VMEM((share_x, share_y, modes_z), jnp.float32),
            dma((tiles, blocks)),
            dma((4,)),
            dma((1,)),
            dma((1,)),
            dma((groups, len(cuts))),
            dma((rights, groups)),
            dma((groups,)),
        ],
        compiler_params=pltpu.CompilerParams(
            collective_id=0, has_side_effects=True, vmem_limit_bytes=62 * 2**20),
    )(signal, table_x, table_y, table_v, table_w, symbol_x, symbol_y[None, :], symbol_z[None, :])


def solution(mesh):
    lefts, rights = mesh.shape["left"], mesh.shape["right"]
    in_specs = (P(None, "left", "right"), P(), P(), P())
    out_specs = P("left", "right", None)
    return jax.shard_map(
        functools.partial(body, lefts, rights), mesh=mesh, in_specs=in_specs, out_specs=out_specs, check_vma=False)
```
